32 devices in a mesh: tm: 8 (over z, x), space: 4 (over y, core).
Axes of the slice: x: 2, y: 2, z: 4, core: 2. Of those that a mesh axis runs over, the one named last changes fastest.
Arguments:
- u_old: float32 [8, 5, 256, 16, 128], P('tm', None, 'space'), may hold values from -2.5 to 2.5
- u_init: float32 [256, 16, 128], P('space'), may hold values from -2.5 to 2.5
Outputs:
- u_new: float32 [8, 5, 256, 16, 128], P('tm', None, 'space')
The draws below stay inside these ranges and needn't reach their ends.
All inputs are finite; a program needn't handle non-finite values.
Results may differ from the reference program's by a relative error of at most 0.0003.
Values sent between devices are 32-bit elements; how exact they have to be, the bound alone decides.
A program may use at most 128 MiB of HBM per device.

```python
import math
import jax
import jax.numpy as jnp
from jax import lax

NZ = 256
NX = 16
NY = 128
FINE_NODES = 5
SLICES = 8
N_TM = 8


def steps_of(key, extent, pieces, smallest, high):
    factor_of, own = 1.0, jax.random.fold_in(key, 6)
    for dim, shards_of in pieces:
        draws = jnp.exp(jax.random.uniform(jax.random.fold_in(own, dim), (shards_of,), jnp.float32, smallest / len(pieces), high / len(pieces)))
        factor_of = factor_of * jnp.repeat(draws, extent[dim] // shards_of).reshape([-1 if axis == dim else 1 for axis in range(len(extent))])
    return factor_of


def bell_draw(own_key, extent, spread, most, split=(), held_as=jnp.bfloat16):
    drawn = jax.random.normal(own_key, extent, jnp.float32) * spread
    if len(split) > 0:
        drawn = steps_of(own_key, extent, split, -0.22, 0.18) * drawn
    return jnp.clip(drawn, min=-most, max=most).astype(held_as)


def setup_inputs(seed: int = 0) -> dict:
    key_of = jax.random.split(jax.random.key(seed), 3)
    return {
        "u_old": bell_draw(key_of[0], (SLICES, FINE_NODES, NZ, NX, NY), 0.6, 2.5, ((0, 8), (2, 4)), jnp.float32),
        "u_init": bell_draw(key_of[1], (NZ, NX, NY), 0.6, 2.5, ((0, 4),), jnp.float32),
    }


step_length = 0.4
diffusion = 1.0
reaction = 1.0

def basis_coefficients(nodes, chosen):
    polynomial = [1.0]
    for other, point in enumerate(nodes):
        if other == chosen:
            continue
        divisor = nodes[chosen] - point
        widened = [0.0] * (len(polynomial) + 1)
        for power, value in enumerate(polynomial):
            widened[power + 1] += value / divisor
            widened[power] -= value * point / divisor
        polynomial = widened
    return polynomial

def basis_value(nodes, chosen, where):
    result = 1.0
    for other, point in enumerate(nodes):
        if other != chosen:
            result *= (where - point) / (nodes[chosen] - point)
    return result

def node_tables():
    root = math.sqrt(3.0 / 7.0)
    fine_tau = [0.0, (1.0 - root) / 2.0, 0.5, (1.0 + root) / 2.0, 1.0]
    coarse_tau = [0.0, 0.5, 1.0]
    integ = []
    for j in range(4):
        row_values = []
        for k in range(5):
            polynomial = basis_coefficients(fine_tau, k)
            total = 0.0
            for power, value in enumerate(polynomial):
                total += value * (fine_tau[j + 1] ** (power + 1) - fine_tau[j] ** (power + 1)) / (power + 1)
            row_values.append(total)
        integ.append(row_values)
    interp = [[basis_value(coarse_tau, c, fine_tau[m]) for c in range(3)] for m in range(5)]
    spacing = [float(fine_tau[j + 1] - fine_tau[j]) for j in range(4)]
    return (jnp.asarray(integ, jnp.float32), spacing, jnp.asarray(interp, jnp.float32))

def fine_force(field):
    near = jnp.roll(field, 1, 0) + jnp.roll(field, -1, 0) + jnp.roll(field, 1, 1) + jnp.roll(field, -1, 1)
    near = near + jnp.roll(field, 1, 2) + jnp.roll(field, -1, 2)
    return diffusion * (near - 6.0 * field) + reaction * (field - field * field * field)

def coarse_lap(field):
    near = jnp.roll(field, 1, 0) + jnp.roll(field, -1, 0) + jnp.roll(field, 1, 1) + jnp.roll(field, -1, 1)
    near = near + jnp.roll(field, 1, 2) + jnp.roll(field, -1, 2)
    return 0.25 * (near - 6.0 * field)

def restrict(field):
    depth, rows, cols = field.shape
    return field.reshape(depth // 2, 2, rows // 2, 2, cols // 2, 2).mean(axis=(1, 3, 5))

def reference(u_old, u_init):
    integ, spacing, interp = node_tables()
    depth_c, rows_c, cols_c = (NZ // 2, NX // 2, NY // 2)
    angle_z = 2.0 * jnp.cos(2.0 * jnp.pi * jnp.arange(depth_c, dtype=jnp.float32) / depth_c)
    angle_x = 2.0 * jnp.cos(2.0 * jnp.pi * jnp.arange(rows_c, dtype=jnp.float32) / rows_c)
    angle_y = 2.0 * jnp.cos(2.0 * jnp.pi * jnp.arange(cols_c, dtype=jnp.float32) / cols_c)
    eigen = 0.25 * (angle_z[:, None, None] + angle_x[None, :, None] + angle_y[None, None, :] - 6.0)
    denom = 1.0 - 0.5 * step_length * diffusion * eigen

    def solve(right):
        return jnp.real(jnp.fft.ifftn(jnp.fft.fftn(right) / denom)).astype(jnp.float32)
    carry = restrict(u_init)
    results = []
    for slice_index in range(N_TM):
        fine_old = u_old[slice_index]
        start = u_init if slice_index == 0 else u_old[slice_index - 1, 4]
        fold = jnp.stack([fine_force(fine_old[k]) for k in range(5)])
        iold = step_length * jnp.einsum('jk,kzxy->jzxy', integ, fold, precision=lax.Precision.HIGHEST)
        states = [start]
        forces = []
        for section in range(4):
            force_now = fine_force(states[section])
            forces.append(force_now)
            states.append(states[section] + step_length * spacing[section] * (force_now - fold[section]) + iold[section])
        forces.append(fine_force(states[4]))
        inew = step_length * jnp.einsum('jk,kzxy->jzxy', integ, jnp.stack(forces), precision=lax.Precision.HIGHEST)
        coarse = [restrict(states[0]), restrict(states[2]), restrict(states[4])]
        lifted0 = restrict(inew[0] + inew[1]) - 0.5 * step_length * diffusion * coarse_lap(coarse[1])
        lifted1 = restrict(inew[2] + inew[3]) - 0.5 * step_length * diffusion * coarse_lap(coarse[2])
        begin = carry
        middle = solve(begin + lifted0)
        finish = solve(middle + lifted1)
        carry = finish
        delta = jnp.stack([begin - coarse[0], middle - coarse[1], finish - coarse[2]])
        timed = jnp.einsum('mc,czxy->mzxy', interp, delta, precision=lax.Precision.HIGHEST)
        upper = jnp.repeat(jnp.repeat(jnp.repeat(timed, 2, 1), 2, 2), 2, 3)
        results.append(jnp.stack(states) + upper)
    return jnp.stack(results)
```

```python
import functools
import math

import jax
import jax.numpy as jnp
import numpy as np
from jax import lax
from jax.experimental import pallas as pl
from jax.experimental.pallas import tpu as pltpu
from jax.sharding import PartitionSpec as P

step_length = 0.4
diffusion = 1.0
reaction = 1.0
HALO = 5
BLOCK = 4
MESH = pl.DeviceIdType.MESH


def basis_coefficients(nodes, chosen):
    polynomial = [1.0]
    for other, point in enumerate(nodes):
        if other == chosen:
            continue
        divisor = nodes[chosen] - point
        widened = [0.0] * (len(polynomial) + 1)
        for power, value in enumerate(polynomial):
            widened[power + 1] += value / divisor
            widened[power] -= value * point / divisor
        polynomial = widened
    return polynomial


def basis_value(nodes, chosen, where):
    result = 1.0
    for other, point in enumerate(nodes):
        if other != chosen:
            result *= (where - point) / (nodes[chosen] - point)
    return result


def node_tables():
    root = math.sqrt(3.0 / 7.0)
    fine_tau = [0.0, (1.0 - root) / 2.0, 0.5, (1.0 + root) / 2.0, 1.0]
    coarse_tau = [0.0, 0.5, 1.0]
    integ = []
    for j in range(4):
        row_values = []
        for k in range(5):
            polynomial = basis_coefficients(fine_tau, k)
            total = 0.0
            for power, value in enumerate(polynomial):
                total += (
                    value
                    * (fine_tau[j + 1] ** (power + 1) - fine_tau[j] ** (power + 1))
                    / (power + 1)
                )
            row_values.append(total)
        integ.append(row_values)
    interp = [[basis_value(coarse_tau, c, fine_tau[m]) for c in range(3)] for m in range(5)]
    spacing = [float(fine_tau[j + 1] - fine_tau[j]) for j in range(4)]
    return integ, spacing, interp


def hartley(length):
    counter = np.arange(length)
    phase = 2.0 * np.pi * (counter[:, None] * counter[None, :] % length) / length
    return (np.cos(phase) + np.sin(phase)) / math.sqrt(length)


def two_parts(table):
    upper = table.astype(jnp.bfloat16)
    lower = (table - upper.astype(np.float64)).astype(jnp.bfloat16)
    return np.stack([upper, lower])


def halves(value):
    upper = value.astype(jnp.bfloat16)
    return upper, (value - upper.astype(jnp.float32)).astype(jnp.bfloat16)


def product(a, b, dims):
    def one(x, y):
        return lax.dot_general(x, y, (dims, ((), ())), preferred_element_type=jnp.float32)

    return one(a[0], b[0]) + (one(a[0], b[1]) + one(a[1], b[0]))


def force(padded):
    field = padded[1:-1]
    rows, cols = field.shape[1:]
    near = padded[2:] + padded[:-2]
    near = near + (pltpu.roll(field, 1, 1) + pltpu.roll(field, rows - 1, 1))
    near = near + (pltpu.roll(field, 1, 2) + pltpu.roll(field, cols - 1, 2))
    linear = reaction - 6.0 * diffusion
    return diffusion * near + field * (linear - reaction * (field * field))


def kernel(
    nt, ns, solvers,
    u_hbm, init_hbm, tab_hbm, ztab_hbm, inv_hbm,
    w_out, timed_out,
    u, w, corr, acc, restricted, tab, ztab, inv,
    send_1, recv_1, send_2, recv_2, up,
    load_sem, table_sem, out_sem, start_sem, halo_send, halo_recv, start_send, start_recv,
    sems,
):
    integ, spacing, interp = node_tables()
    h = step_length
    devices = nt * ns
    depth, rows, cols = init_hbm.shape
    depth_c, rows_c = depth // 2, rows // 2
    length = send_1.shape[2]
    modes = send_1.shape[1]
    own = pl.ds(HALO, depth)
    t, s = lax.axis_index("tm"), lax.axis_index("space")
    me = t * ns + s
    above, below = lax.rem(s + 1, ns), lax.rem(s + ns - 1, ns)

    barrier = pltpu.get_barrier_semaphore()

    def greet(i, carry):
        other = lax.rem(me + i, devices)
        pl.semaphore_signal(
            barrier, inc=1, device_id=(other // ns, lax.rem(other, ns)), device_id_type=MESH
        )
        return carry

    lax.fori_loop(1, devices, greet, 0)
    load = pltpu.make_async_copy(u_hbm.at[0], u.at[:, own], load_sem)
    load.start()
    tables = [
        pltpu.make_async_copy(source, target, table_sem.at[i])
        for i, (source, target) in enumerate(((tab_hbm, tab), (ztab_hbm, ztab), (inv_hbm, inv)))
    ]
    for copy in tables:
        copy.start()
    local_start = pltpu.make_async_copy(init_hbm, w.at[0, own], start_sem)

    @pl.when(t == 0)
    def _():
        local_start.start()

    pl.semaphore_wait(barrier, devices - 1)

    lows, highs = pl.ds(0, HALO), pl.ds(HALO + depth, HALO)
    first, last = pl.ds(0, HALO), pl.ds(depth - HALO, HALO)

    def remote(source, target, send, recv, place):
        return pltpu.make_async_remote_copy(
            src_ref=source, dst_ref=target, send_sem=send, recv_sem=recv,
            device_id=place, device_id_type=MESH,
        )

    after = jnp.minimum(t + 1, nt - 1)
    node = u_hbm.at[0, 4]
    starts = [
        remote(node, w.at[0, own], start_send.at[0], start_recv.at[0], (after, s)),
        remote(node.at[last], w.at[0, lows], start_send.at[1], start_recv.at[1], (after, above)),
        remote(node.at[first], w.at[0, highs], start_send.at[2], start_recv.at[2], (after, below)),
    ]
    inits = [
        remote(init_hbm.at[last], w.at[0, lows], start_send.at[3], start_recv.at[1], (t, above)),
        remote(init_hbm.at[first], w.at[0, highs], start_send.at[4], start_recv.at[2], (t, below)),
    ]
    halos = [
        remote(u_hbm.at[0, :, last], u.at[:, lows], halo_send.at[0], halo_recv.at[0], (t, above)),
        remote(u_hbm.at[0, :, first], u.at[:, highs], halo_send.at[1], halo_recv.at[1], (t, below)),
    ]
    for copy in halos:
        copy.start()

    @pl.when(t < nt - 1)
    def _():
        for copy in starts:
            copy.start()

    @pl.when(t == 0)
    def _():
        for copy in inits:
            copy.start()

    load.wait()
    for copy in halos:
        copy.wait_recv()

    blocks = (depth + 2 * HALO - 2) // BLOCK

    def fold_block(i, carry):
        z = 1 + i * BLOCK
        forces = [force(u[k, pl.ds(z - 1, BLOCK + 2)]) for k in range(5)]
        for j in range(4):
            total = None
            for k in range(5):
                weight = h * integ[j][k] - (h * spacing[j] if j == k else 0.0)
                term = weight * forces[k]
                total = term if total is None else total + term
            corr[j, pl.ds(z, BLOCK)] = total
        return carry

    lax.fori_loop(0, blocks, fold_block, 0)

    @pl.when(t == 0)
    def _():
        local_start.wait()

    @pl.when(t > 0)
    def _():
        starts[0].wait_recv()

    starts[1].wait_recv()
    starts[2].wait_recv()

    for m in range(4):
        def sweep_block(i, carry, m=m):
            z = 1 + i * BLOCK
            here = pl.ds(z, BLOCK)
            padded = w[m, pl.ds(z - 1, BLOCK + 2)]
            now = force(padded)
            w[m + 1, here] = padded[1:-1] + (h * spacing[m]) * now + corr[m, here]
            for a in range(2):
                term = (h * (integ[2 * a][m] + integ[2 * a + 1][m])) * now
                acc[a, here] = term if m == 0 else acc[a, here] + term
            return carry

        lax.fori_loop(0, blocks, sweep_block, 0)

    write = pltpu.make_async_copy(w.at[:, own], w_out, out_sem)
    write.start()

    plane = rows * depth_c

    def last_block(i, carry):
        z = HALO + i * BLOCK
        here = pl.ds(z, BLOCK)
        padded = w[4, pl.ds(z - 1, BLOCK + 2)]
        now, end = force(padded), padded[1:-1]
        middle = w[2, here]
        outs = []
        for a in range(2):
            term = acc[a, here] + (h * (integ[2 * a][4] + integ[2 * a + 1][4])) * now
            outs.append(term + ((w[0, here] - middle) if a == 0 else (middle - end)))
        outs.append(end - u[4, here])
        for f in range(3):
            pair = outs[f].reshape(BLOCK // 2, 2, rows, cols)
            pair = pair[:, 0] + pair[:, 1]
            place = pl.multiple_of(f * plane + i * (BLOCK // 2) * rows, 8)
            restricted[pl.ds(place, BLOCK // 2 * rows), :] = pair.reshape(BLOCK // 2 * rows, cols)
        return carry

    lax.fori_loop(0, depth // BLOCK, last_block, 0)

    filled = 3 * depth_c
    pieces = []
    for x in range(rows_c):
        even = restricted[pl.ds(2 * x, filled, stride=rows), :]
        odd = restricted[pl.ds(2 * x + 1, filled, stride=rows), :]
        pieces.append((even + odd) * 0.125)
    flat = jnp.concatenate(pieces, axis=1)
    if length > filled:
        flat = jnp.concatenate([flat, jnp.zeros((length - filled, rows_c * cols), jnp.float32)], axis=0)
    for copy in tables:
        copy.wait()
    spectral = product((tab[0], tab[1]), halves(flat), ((1,), (1,)))
    send_1[...] = spectral.reshape(solvers, modes, length)

    slot = s * nt + t

    def spread(i, carry):
        other = lax.rem(me + i, solvers)

        @pl.when(other != me)
        def _():
            remote(
                send_1.at[other], recv_1.at[slot], sems.at[0], sems.at[1],
                (other // ns, lax.rem(other, ns)),
            ).start()

        return carry

    lax.fori_loop(0, solvers, spread, 0)

    def when_all(condition, body):
        if solvers == devices:
            body()
        else:
            pl.when(condition)(body)

    def bytes_wait(ref, count, sem):
        part = ref.at[pl.ds(0, count)]
        pltpu.make_async_copy(part, part, sem).wait()

    def solve():
        recv_1[slot] = send_1[me]
        bytes_wait(recv_1, devices - 1, sems.at[1])
        joined = jnp.concatenate(
            [recv_1[pl.ds(q * nt, nt)].reshape(nt * modes, length) for q in range(ns)], axis=1
        )
        spectra = product(halves(joined), (ztab[0], ztab[1]), ((1,), (0,)))
        width = inv.shape[1]
        factor = inv[pl.ds(pl.multiple_of(me * modes, 8), modes), :]
        begin = jnp.zeros((modes, width), jnp.float32)
        rows_of = []
        for n in range(nt):
            part = spectra[n * modes:(n + 1) * modes]
            middle = (begin + part[:, :width]) * factor
            finish = (middle + part[:, width:2 * width]) * factor
            rows_of.append(jnp.concatenate([begin, middle, finish], axis=1))
            begin = finish + part[:, 2 * width:]
        solved = jnp.concatenate(rows_of, axis=0)
        back = product(halves(solved), (ztab[0], ztab[1]), ((1,), (1,)))
        for q in range(ns):
            send_2[pl.ds(q * nt, nt)] = back[:, q * length:(q + 1) * length].reshape(nt, modes, length)

        def give(i, carry):
            other = lax.rem(me + i, devices)
            to_t, to_s = other // ns, lax.rem(other, ns)
            remote(
                send_2.at[to_s * nt + to_t], recv_2.at[me], sems.at[2], sems.at[3], (to_t, to_s)
            ).start()
            return carry

        lax.fori_loop(1, devices, give, 0)
        recv_2[me] = send_2[slot]
        bytes_wait(recv_2, solvers - 1, sems.at[3])

    when_all(me < solvers, solve)
    if solvers != devices:
        @pl.when(me >= solvers)
        def _():
            bytes_wait(recv_2, solvers, sems.at[3])

    delta = jnp.transpose(recv_2[...].reshape(solvers * modes, length))[:filled]
    coarse = product(halves(delta), (tab[0], tab[1]), ((1,), (0,)))
    for x in range(rows_c):
        part = coarse[:, x * cols:(x + 1) * cols]
        for side in range(2):
            up[pl.ds(2 * x + side, filled, stride=rows), :] = part
    for m in range(5):
        total = None
        for c in range(3):
            if abs(interp[m][c]) < 1e-14:
                continue
            term = up[pl.ds(c * plane, plane), :]
            if abs(interp[m][c] - 1.0) > 1e-14:
                term = interp[m][c] * term
            total = term if total is None else total + term
        timed_out[m] = total.reshape(depth_c, rows, cols)

    write.wait()
    for copy in halos:
        copy.wait_send()

    @pl.when(t < nt - 1)
    def _():
        for copy in starts:
            copy.wait_send()

    @pl.when(t == 0)
    def _():
        for copy in inits:
            copy.wait_send()

    def sent():
        bytes_wait(send_1, solvers - 1, sems.at[0])
        bytes_wait(send_2, devices - 1, sems.at[2])

    when_all(me < solvers, sent)
    if solvers != devices:
        @pl.when(me >= solvers)
        def _():
            bytes_wait(send_1, solvers, sems.at[0])


def shards(nt, ns, u_old, u_init):
    depth, rows, cols = u_init.shape
    depth_c, rows_c, cols_c = depth // 2, rows // 2, cols // 2
    whole_c = depth_c * ns
    count = rows_c * cols_c
    devices = nt * ns
    solvers = min(devices, count // 8)
    modes = count // solvers
    length = -(-3 * depth_c // 128) * 128
    extended = depth + 2 * HALO

    wide = np.repeat(hartley(cols_c), 2, axis=1)
    tab = two_parts(np.kron(hartley(rows_c), wide))
    wave = hartley(whole_c)
    ztab = np.zeros((ns, length, 3 * whole_c))
    for f in range(3):
        ztab[:, f * depth_c:(f + 1) * depth_c, f * whole_c:(f + 1) * whole_c] = wave.reshape(ns, depth_c, whole_c)
    ztab = two_parts(ztab.reshape(ns * length, 3 * whole_c))
    angle_z = 2.0 * np.cos(2.0 * np.pi * np.arange(whole_c) / whole_c)
    angle_x = 2.0 * np.cos(2.0 * np.pi * np.arange(rows_c) / rows_c)
    angle_y = 2.0 * np.cos(2.0 * np.pi * np.arange(cols_c) / cols_c)
    planar = (angle_x[:, None] + angle_y[None, :]).reshape(count)
    eigen = 0.25 * (planar[:, None] + angle_z[None, :] - 6.0)
    inv = (1.0 / (1.0 - 0.5 * step_length * diffusion * eigen)).astype(np.float32)

    anywhere = pl.BlockSpec(memory_space=pl.ANY)
    f32 = jnp.float32
    w, timed = pl.pallas_call(
        functools.partial(kernel, nt, ns, solvers),
        out_shape=(
            jax.ShapeDtypeStruct((5, depth, rows, cols), f32),
            jax.ShapeDtypeStruct((5, depth_c, rows, cols), f32),
        ),
        in_specs=[anywhere] * 5,
        out_specs=(anywhere, pl.BlockSpec(memory_space=pltpu.VMEM)),
        scratch_shapes=[
            pltpu.VMEM((5, extended, rows, cols), f32),
            pltpu.VMEM((5, extended, rows, cols), f32),
            pltpu.VMEM((4, extended, rows, cols), f32),
            pltpu.VMEM((2, extended, rows, cols), f32),
            pltpu.VMEM((3 * depth_c * rows, cols), f32),
            pltpu.VMEM(tab.shape, jnp.bfloat16),
            pltpu.VMEM(ztab.shape, jnp.bfloat16),
            pltpu.VMEM(inv.shape, f32),
            pltpu.VMEM((solvers, modes, length), f32),
            pltpu.VMEM((devices, modes, length), f32),
            pltpu.VMEM((devices, modes, length), f32),
            pltpu.VMEM((solvers, modes, length), f32),
            pltpu.VMEM((3 * depth_c * rows, cols), f32),
            pltpu.SemaphoreType.DMA,
            pltpu.SemaphoreType.DMA((3,)),
            pltpu.SemaphoreType.DMA,
            pltpu.SemaphoreType.DMA,
            pltpu.SemaphoreType.DMA((2,)),
            pltpu.SemaphoreType.DMA((2,)),
            pltpu.SemaphoreType.DMA((5,)),
            pltpu.SemaphoreType.DMA((3,)),
            pltpu.SemaphoreType.DMA((4,)),
        ],
        compiler_params=pltpu.CompilerParams(
            collective_id=0, has_side_effects=True, vmem_limit_bytes=48 * 1024 * 1024
        ),
    )(u_old, u_init, tab, ztab, inv)
    result = w.reshape(5, depth_c, 2, rows, cols) + timed[:, :, None]
    return result.reshape(1, 5, depth, rows, cols)


def solution(mesh):
    return jax.shard_map(
        functools.partial(shards, mesh.shape["tm"], mesh.shape["space"]),
        mesh=mesh,
        in_specs=(P("tm", None, "space", None, None), P("space", None, None)),
        out_specs=P("tm", None, "space", None, None),
        check_vma=False,
    )
```

```python
import functools
import math

import jax
import jax.numpy as jnp
import numpy as np
from jax import lax
from jax.experimental import pallas as pl
from jax.experimental.pallas import tpu as pltpu
from jax.sharding import PartitionSpec as P

step_length = 0.4
diffusion = 1.0
reaction = 1.0
HALO = 5
BLOCK = 4
MESH = pl.DeviceIdType.MESH


def basis_coefficients(nodes, chosen):
    polynomial = [1.0]
    for other, point in enumerate(nodes):
        if other == chosen:
            continue
        divisor = nodes[chosen] - point
        widened = [0.0] * (len(polynomial) + 1)
        for power, value in enumerate(polynomial):
            widened[power + 1] += value / divisor
            widened[power] -= value * point / divisor
        polynomial = widened
    return polynomial


def basis_value(nodes, chosen, where):
    result = 1.0
    for other, point in enumerate(nodes):
        if other != chosen:
            result *= (where - point) / (nodes[chosen] - point)
    return result


def node_tables():
    root = math.sqrt(3.0 / 7.0)
    fine_tau = [0.0, (1.0 - root) / 2.0, 0.5, (1.0 + root) / 2.0, 1.0]
    coarse_tau = [0.0, 0.5, 1.0]
    integ = []
    for j in range(4):
        row_values = []
        for k in range(5):
            polynomial = basis_coefficients(fine_tau, k)
            total = 0.0
            for power, value in enumerate(polynomial):
                total += (
                    value
                    * (fine_tau[j + 1] ** (power + 1) - fine_tau[j] ** (power + 1))
                    / (power + 1)
                )
            row_values.append(total)
        integ.append(row_values)
    interp = [[basis_value(coarse_tau, c, fine_tau[m]) for c in range(3)] for m in range(5)]
    spacing = [float(fine_tau[j + 1] - fine_tau[j]) for j in range(4)]
    return integ, spacing, interp


def hartley(length):
    counter = np.arange(length)
    phase = 2.0 * np.pi * (counter[:, None] * counter[None, :] % length) / length
    return (np.cos(phase) + np.sin(phase)) / math.sqrt(length)


def two_parts(table):
    upper = table.astype(jnp.bfloat16)
    lower = (table - upper.astype(np.float64)).astype(jnp.bfloat16)
    return np.stack([upper, lower])


def halves(value):
    upper = value.astype(jnp.bfloat16)
    return upper, (value - upper.astype(jnp.float32)).astype(jnp.bfloat16)


def product(a, b, dims):
    def one(x, y):
        return lax.dot_general(x, y, (dims, ((), ())), preferred_element_type=jnp.float32)

    return one(a[0], b[0]) + (one(a[0], b[1]) + one(a[1], b[0]))


def force(padded):
    field = padded[1:-1]
    rows, cols = field.shape[1:]
    near = padded[2:] + padded[:-2]
    near = near + (pltpu.roll(field, 1, 1) + pltpu.roll(field, rows - 1, 1))
    near = near + (pltpu.roll(field, 1, 2) + pltpu.roll(field, cols - 1, 2))
    linear = reaction - 6.0 * diffusion
    return diffusion * near + field * (linear - reaction * (field * field))


def kernel(
    nt, ns, solvers,
    u_hbm, init_hbm, tab_hbm, ztab_hbm, inv_hbm,
    out,
    u, w, corr, acc, restricted, tab, ztab, inv,
    send_1, recv_1, send_2, recv_2, up,
    load_sem, table_sem, start_sem, halo_send, halo_recv, start_send, start_recv,
    sems, known_sem,
):
    integ, spacing, interp = node_tables()
    h = step_length
    devices = nt * ns
    depth, rows, cols = init_hbm.shape
    depth_c, rows_c = depth // 2, rows // 2
    length = send_1.shape[2]
    modes = send_1.shape[1]
    own = pl.ds(HALO, depth)
    t, s = lax.axis_index("tm"), lax.axis_index("space")
    me = t * ns + s
    above, below = lax.rem(s + 1, ns), lax.rem(s + ns - 1, ns)

    barrier = pltpu.get_barrier_semaphore()

    def signal_along(sem, step):
        @pl.when(t + step < nt)
        def _():
            pl.semaphore_signal(sem, inc=1, device_id=(t + step, s), device_id_type=MESH)

        @pl.when(t >= step)
        def _():
            pl.semaphore_signal(sem, inc=1, device_id=(t - step, s), device_id_type=MESH)

    def sides(step):
        return jnp.where(t + step < nt, 1, 0) + jnp.where(t >= step, 1, 0)

    signal_along(barrier, 1)
    for i in range(1, ns):
        pl.semaphore_signal(
            barrier, inc=1, device_id=(t, lax.rem(s + i, ns)), device_id_type=MESH
        )
    load = pltpu.make_async_copy(u_hbm.at[0], u.at[:, own], load_sem)
    load.start()
    tables = [
        pltpu.make_async_copy(source, target, table_sem.at[i])
        for i, (source, target) in enumerate(((tab_hbm, tab), (ztab_hbm, ztab), (inv_hbm, inv)))
    ]
    for copy in tables:
        copy.start()
    local_start = pltpu.make_async_copy(init_hbm, w.at[0, own], start_sem)

    @pl.when(t == 0)
    def _():
        local_start.start()

    pl.semaphore_wait(barrier, ns - 1 + sides(1))

    lows, highs = pl.ds(0, HALO), pl.ds(HALO + depth, HALO)
    first, last = pl.ds(0, HALO), pl.ds(depth - HALO, HALO)

    def remote(source, target, send, recv, place):
        return pltpu.make_async_remote_copy(
            src_ref=source, dst_ref=target, send_sem=send, recv_sem=recv,
            device_id=place, device_id_type=MESH,
        )

    after = jnp.minimum(t + 1, nt - 1)
    node = u_hbm.at[0, 4]
    cuts = [(0, HALO), (depth - HALO, HALO), (HALO, depth - 2 * HALO)]
    starts = [
        remote(
            node.at[pl.ds(begin, size)], w.at[0, pl.ds(HALO + begin, size)],
            start_send.at[i], start_recv.at[i], (after, s),
        )
        for i, (begin, size) in enumerate(cuts)
    ]

    def edges(source, shift):
        return [
            remote(
                source.at[pl.ds(shift + depth - HALO, HALO)], w.at[0, lows],
                start_send.at[3], start_recv.at[3], (t, above),
            ),
            remote(
                source.at[pl.ds(shift, HALO)], w.at[0, highs],
                start_send.at[4], start_recv.at[4], (t, below),
            ),
        ]

    inits, passed = edges(init_hbm, 0), edges(w.at[0], HALO)
    halos = [
        remote(u_hbm.at[0, :, last], u.at[:, lows], halo_send.at[0], halo_recv.at[0], (t, above)),
        remote(u_hbm.at[0, :, first], u.at[:, highs], halo_send.at[1], halo_recv.at[1], (t, below)),
    ]
    @pl.when(t < nt - 1)
    def _():
        for copy in starts:
            copy.start()

    for copy in halos:
        copy.start()

    @pl.when(t == 0)
    def _():
        for copy in inits:
            copy.start()

    signal_along(known_sem.at[0], 1)
    load.wait()
    for copy in halos:
        copy.wait_recv()

    blocks = (depth + 2 * HALO - 2) // BLOCK

    def fold_block(i, carry):
        z = 1 + i * BLOCK
        forces = [force(u[k, pl.ds(z - 1, BLOCK + 2)]) for k in range(5)]
        for j in range(4):
            total = None
            for k in range(5):
                weight = h * integ[j][k] - (h * spacing[j] if j == k else 0.0)
                term = weight * forces[k]
                total = term if total is None else total + term
            corr[j, pl.ds(z, BLOCK)] = total
        return carry

    lax.fori_loop(0, blocks, fold_block, 0)

    @pl.when(t == 0)
    def _():
        local_start.wait()

    @pl.when(t > 0)
    def _():
        starts[1].wait_recv()
        passed[0].start()
        starts[0].wait_recv()
        passed[1].start()

    for i in range(known_sem.shape[0]):
        if i > 0:
            signal_along(known_sem.at[i], 2 ** i)
        pl.semaphore_wait(known_sem.at[i], sides(2 ** i))

    @pl.when(t > 0)
    def _():
        starts[2].wait_recv()

    for copy in inits:
        copy.wait_recv()

    for m in range(4):
        def sweep_block(i, carry, m=m):
            z = 1 + i * BLOCK
            here = pl.ds(z, BLOCK)
            padded = w[m, pl.ds(z - 1, BLOCK + 2)]
            now = force(padded)
            w[m + 1, here] = padded[1:-1] + (h * spacing[m]) * now + corr[m, here]
            for a in range(2):
                term = (h * (integ[2 * a][m] + integ[2 * a + 1][m])) * now
                acc[a, here] = term if m == 0 else acc[a, here] + term
            return carry

        lax.fori_loop(0, blocks, sweep_block, 0)

    plane = rows * depth_c

    def last_block(i, carry):
        z = HALO + i * BLOCK
        here = pl.ds(z, BLOCK)
        padded = w[4, pl.ds(z - 1, BLOCK + 2)]
        now, end = force(padded), padded[1:-1]
        middle = w[2, here]
        outs = []
        for a in range(2):
            term = acc[a, here] + (h * (integ[2 * a][4] + integ[2 * a + 1][4])) * now
            outs.append(term + ((w[0, here] - middle) if a == 0 else (middle - end)))
        outs.append(end - u[4, here])
        for f in range(3):
            pair = outs[f].reshape(BLOCK // 2, 2, rows, cols)
            pair = pair[:, 0] + pair[:, 1]
            place = pl.multiple_of(f * plane + i * (BLOCK // 2) * rows, 8)
            restricted[pl.ds(place, BLOCK // 2 * rows), :] = pair.reshape(BLOCK // 2 * rows, cols)
        return carry

    lax.fori_loop(0, depth // BLOCK, last_block, 0)

    filled = 3 * depth_c
    pieces = []
    for x in range(rows_c):
        even = restricted[pl.ds(2 * x, filled, stride=rows), :]
        odd = restricted[pl.ds(2 * x + 1, filled, stride=rows), :]
        pieces.append((even + odd) * 0.125)
    flat = jnp.concatenate(pieces, axis=1)
    if length > filled:
        flat = jnp.concatenate([flat, jnp.zeros((length - filled, rows_c * cols), jnp.float32)], axis=0)
    for copy in tables:
        copy.wait()
    spectral = product((tab[0], tab[1]), halves(flat), ((1,), (1,)))
    send_1[...] = spectral.reshape(solvers, modes, length)

    slot = s * nt + t

    def spread(i, carry):
        other = lax.rem(me + i, solvers)

        @pl.when(other != me)
        def _():
            remote(
                send_1.at[other], recv_1.at[slot], sems.at[0], sems.at[1],
                (other // ns, lax.rem(other, ns)),
            ).start()

        return carry

    lax.fori_loop(0, solvers, spread, 0)

    def when_all(condition, body):
        if solvers == devices:
            body()
        else:
            pl.when(condition)(body)

    def bytes_wait(ref, count, sem):
        part = ref.at[pl.ds(0, count)]
        pltpu.make_async_copy(part, part, sem).wait()

    def solve():
        recv_1[slot] = send_1[me]
        bytes_wait(recv_1, devices - 1, sems.at[1])
        joined = jnp.concatenate(
            [recv_1[pl.ds(q * nt, nt)].reshape(nt * modes, length) for q in range(ns)], axis=1
        )
        spectra = product(halves(joined), (ztab[0], ztab[1]), ((1,), (0,)))
        width = inv.shape[1]
        factor = inv[pl.ds(pl.multiple_of(me * modes, 8), modes), :]
        begin = jnp.zeros((modes, width), jnp.float32)
        rows_of = []
        for n in range(nt):
            part = spectra[n * modes:(n + 1) * modes]
            middle = (begin + part[:, :width]) * factor
            finish = (middle + part[:, width:2 * width]) * factor
            rows_of.append(jnp.concatenate([begin, middle, finish], axis=1))
            begin = finish + part[:, 2 * width:]
        solved = jnp.concatenate(rows_of, axis=0)
        back = product(halves(solved), (ztab[0], ztab[1]), ((1,), (1,)))
        for q in range(ns):
            send_2[pl.ds(q * nt, nt)] = back[:, q * length:(q + 1) * length].reshape(nt, modes, length)

        def give(i, carry):
            other = lax.rem(me + i, devices)
            to_t, to_s = other // ns, lax.rem(other, ns)
            remote(
                send_2.at[to_s * nt + to_t], recv_2.at[me], sems.at[2], sems.at[3], (to_t, to_s)
            ).start()
            return carry

        lax.fori_loop(1, devices, give, 0)
        recv_2[me] = send_2[slot]
        bytes_wait(recv_2, solvers - 1, sems.at[3])

    when_all(me < solvers, solve)
    if solvers != devices:
        @pl.when(me >= solvers)
        def _():
            bytes_wait(recv_2, solvers, sems.at[3])

    delta = jnp.transpose(recv_2[...].reshape(solvers * modes, length))[:filled]
    coarse = product(halves(delta), (tab[0], tab[1]), ((1,), (0,)))
    for x in range(rows_c):
        part = coarse[:, x * cols:(x + 1) * cols]
        for side in range(2):
            up[pl.ds(2 * x + side, filled, stride=rows), :] = part

    def add_block(i, carry):
        fields = [
            up[pl.ds(pl.multiple_of(c * plane + i * (BLOCK // 2) * rows, 8), BLOCK // 2 * rows), :]
            for c in range(3)
        ]
        for m in range(5):
            total = None
            for c in range(3):
                if abs(interp[m][c]) < 1e-14:
                    continue
                term = fields[c]
                if abs(interp[m][c] - 1.0) > 1e-14:
                    term = interp[m][c] * term
                total = term if total is None else total + term
            total = total.reshape(BLOCK // 2, 1, rows, cols)
            total = jnp.broadcast_to(total, (BLOCK // 2, 2, rows, cols)).reshape(BLOCK, rows, cols)
            z = i * BLOCK
            out[0, m, pl.ds(z, BLOCK)] = w[m, pl.ds(HALO + z, BLOCK)] + total
        return carry

    lax.fori_loop(0, depth // BLOCK, add_block, 0)

    for copy in halos:
        copy.wait_send()

    @pl.when(t < nt - 1)
    def _():
        for copy in starts:
            copy.wait_send()

    for copy in inits:
        copy.wait_send()

    def sent():
        bytes_wait(send_1, solvers - 1, sems.at[0])
        bytes_wait(send_2, devices - 1, sems.at[2])

    when_all(me < solvers, sent)
    if solvers != devices:
        @pl.when(me >= solvers)
        def _():
            bytes_wait(send_1, solvers, sems.at[0])


def shards(nt, ns, u_old, u_init):
    depth, rows, cols = u_init.shape
    depth_c, rows_c, cols_c = depth // 2, rows // 2, cols // 2
    whole_c = depth_c * ns
    count = rows_c * cols_c
    devices = nt * ns
    solvers = min(devices, count // 8)
    modes = count // solvers
    length = -(-3 * depth_c // 128) * 128
    extended = depth + 2 * HALO
    rounds = max(1, (nt - 1).bit_length())

    wide = np.repeat(hartley(cols_c), 2, axis=1)
    tab = two_parts(np.kron(hartley(rows_c), wide))
    wave = hartley(whole_c)
    ztab = np.zeros((ns, length, 3 * whole_c))
    for f in range(3):
        ztab[:, f * depth_c:(f + 1) * depth_c, f * whole_c:(f + 1) * whole_c] = wave.reshape(ns, depth_c, whole_c)
    ztab = two_parts(ztab.reshape(ns * length, 3 * whole_c))
    angle_z = 2.0 * np.cos(2.0 * np.pi * np.arange(whole_c) / whole_c)
    angle_x = 2.0 * np.cos(2.0 * np.pi * np.arange(rows_c) / rows_c)
    angle_y = 2.0 * np.cos(2.0 * np.pi * np.arange(cols_c) / cols_c)
    planar = (angle_x[:, None] + angle_y[None, :]).reshape(count)
    eigen = 0.25 * (planar[:, None] + angle_z[None, :] - 6.0)
    inv = (1.0 / (1.0 - 0.5 * step_length * diffusion * eigen)).astype(np.float32)

    f32 = jnp.float32
    return pl.pallas_call(
        functools.partial(kernel, nt, ns, solvers),
        out_shape=jax.ShapeDtypeStruct((1, 5, depth, rows, cols), f32),
        in_specs=[pl.BlockSpec(memory_space=pltpu.HBM)] * 5,
        out_specs=pl.BlockSpec(memory_space=pltpu.VMEM),
        scratch_shapes=[
            pltpu.VMEM((5, extended, rows, cols), f32),
            pltpu.VMEM((5, extended, rows, cols), f32),
            pltpu.VMEM((4, extended, rows, cols), f32),
            pltpu.VMEM((2, extended, rows, cols), f32),
            pltpu.VMEM((3 * depth_c * rows, cols), f32),
            pltpu.VMEM(tab.shape, jnp.bfloat16),
            pltpu.VMEM(ztab.shape, jnp.bfloat16),
            pltpu.VMEM(inv.shape, f32),
            pltpu.VMEM((solvers, modes, length), f32),
            pltpu.VMEM((devices, modes, length), f32),
            pltpu.VMEM((devices, modes, length), f32),
            pltpu.VMEM((solvers, modes, length), f32),
            pltpu.VMEM((3 * depth_c * rows, cols), f32),
            pltpu.SemaphoreType.DMA,
            pltpu.SemaphoreType.DMA((3,)),
            pltpu.SemaphoreType.DMA,
            pltpu.SemaphoreType.DMA((2,)),
            pltpu.SemaphoreType.DMA((2,)),
            pltpu.SemaphoreType.DMA((5,)),
            pltpu.SemaphoreType.DMA((5,)),
            pltpu.SemaphoreType.DMA((4,)),
            pltpu.SemaphoreType.REGULAR((rounds,)),
        ],
        compiler_params=pltpu.CompilerParams(
            collective_id=0, has_side_effects=True, vmem_limit_bytes=62000000
        ),
    )(u_old, u_init, tab, ztab, inv)


def solution(mesh):
    return jax.shard_map(
        functools.partial(shards, mesh.shape["tm"], mesh.shape["space"]),
        mesh=mesh,
        in_specs=(P("tm", None, "space", None, None), P("space", None, None)),
        out_specs=P("tm", None, "space", None, None),
        check_vma=False,
    )
```
